32 devices in a mesh: tm: 8 (over z, x), trk: 4 (over y, core).
Axes of the slice: x: 2, y: 2, z: 4, core: 2. Of those that a mesh axis runs over, the one named last changes fastest.
Arguments:
- track_embed: bfloat16 [1024, 1024], P(('tm', 'trk')), may hold values from -6 to 6
- view_ids: int32 [1024, 16], P(('tm', 'trk')), may hold values from 0 to 63, all different within a row; in each aligned block of 32 rows (0 to 31, 32 to 63, ...) at most 16 rows name the same one
- view_count: int32 [1024], P(('tm', 'trk')), may hold values from 1 to 16
- key_feats: bfloat16 [8, 8, 512, 1024], P('tm', 'trk'), may hold values from -160 to 160
- value_feats: bfloat16 [8, 8, 512, 1024], P('tm', 'trk'), may hold values from -6 to 6
- track_gain: float32 [1024], replicated, may hold values from 0.5 to 1.5
- w_temporal: bfloat16 [1024, 3072], replicated, may hold values from -0.1875 to 0.1875
- temporal_scale: float32 [8], replicated, may hold values from 0.5 to 40
- w_merge: bfloat16 [1024, 1024], replicated, may hold values from -0.1875 to 0.1875
- box_gain: float32 [1024], replicated, may hold values from 0.5 to 1.5
- w_hidden: bfloat16 [1024, 512], replicated, may hold values from -0.1875 to 0.1875
- b_hidden: float32 [512], replicated, may hold values from -4 to 4
- w_box: bfloat16 [512, 10], replicated, may hold values from -0.25 to 0.25
Outputs:
- refined: bfloat16 [1024, 16, 1024], P(('tm', 'trk'))
- boxes: float32 [1024, 16, 10], P(('tm', 'trk'))
The draws below stay inside these ranges and needn't reach their ends.
Inputs may be any that keep to these rules, and one draw needn't show every extreme that they name: `view_ids`: entry v stands for frame v // 8 seen by camera v % 8. The 16 entries of one track are distinct. Counting padding entries too, at most 16 of the tracks of one device name any one view, and in some of the devices exactly 16 name one view. Only the first view_count entries of a track's list are visible; the others are padding.
All inputs are finite; a program needn't handle non-finite values.
Results may differ from the reference program's by a relative error of at most 0.0055.
The reference program's roundings to bfloat16 on the way count: a program that leaves them out, or rounds other values in their place, can miss the bound.
Values may be sent and summed in bfloat16 or wider, within the bound.
No kernel may reach another device: no remote copies, remote signals or barrier semaphores. Data moves between devices by JAX's collectives and lax.ppermute only.
A program may use at most 64 MiB of HBM per device.

```python
import math
import jax
import jax.numpy as jnp
import numpy as np
from jax import lax

D = 1024
HEADS = 8
MLPW = 512
BOX = 10
CAMS = 8
VMAX = 16
PIX = 512
TRK_DEV = 32
FR_DEV = 1
FRAMES = 8
TRACKS = 1024
CAP = 16
N_TM = 8
N_TRK = 4


def draw_key_feats(key, part):
    base_draw = jax.random.normal(key, (FRAMES, CAMS, PIX, D), jnp.float32)
    return jnp.clip(base_draw, -6.0, 6.0).astype(jnp.bfloat16)


def draw_temporal_scale(key, part):
    return jax.random.uniform(key, (HEADS,), jnp.float32, 0.5, 2.0)


def plant(drawn, rng, low, largest):
    dims = drawn.shape
    place = [jax.random.randint(jax.random.fold_in(rng, axis), (), 0, dims[axis]) for axis in range(len(dims))]
    drawn = drawn.at[tuple(place)].set(low)
    longest = dims.index(max(dims))
    place[longest] = (place[longest] + 1) % dims[longest]
    return drawn.at[tuple(place)].set(largest)


def levels(own_key, dims, shards, low, top_value):
    def one(axis_at, parts):
        heights = jax.random.uniform(jax.random.fold_in(jax.random.fold_in(own_key, 6), axis_at), (parts,), jnp.float32, low / len(shards), top_value / len(shards))
        return jnp.repeat(jnp.exp(heights), dims[axis_at] // parts).reshape((-1,) + (1,) * (len(dims) - axis_at - 1))

    factor_of = one(*shards[0])
    for cut in shards[1:]:
        factor_of = factor_of * one(*cut)
    return factor_of


def assign_block(rng, own, number, rows, amount, top, reach, lean):
    order = jax.random.permutation(rng, amount)
    crowded, common = shares(amount, rows * top, reach, lean, True), shares(amount, rows * top, reach, lean, False)
    places = jnp.arange(amount)

    def named(sizes, turn):
        used = int((sizes > 0).sum())
        fixed = max(1, used // 4)
        moved = fixed + (places - fixed + turn * (used - fixed)) % max(1, amount - fixed)
        return jnp.zeros((amount,), jnp.int32).at[order[jnp.where(places < fixed, places, moved)]].set(jnp.asarray(sizes, jnp.int32))

    sizes = jnp.where(number % 4 == 0, named(crowded, number // 4), named(common, number - number // 4 - 1))
    mixed = jax.random.permutation(jax.random.fold_in(own, 3), amount)
    donor, sink = mixed[0:amount // 2 * 2:2], mixed[1:amount // 2 * 2:2]
    margin = jnp.minimum(sizes[donor] - 1, reach - sizes[sink]) // 2
    margin = jnp.where((donor == order[0]) | (sink == order[0]) | (sizes[sink] == 0), 0, jnp.maximum(margin, 0))
    moved = jax.random.randint(jax.random.fold_in(own, 4), (amount // 2,), 0, 1 << 20) % (margin + 1)
    sizes = sizes.at[donor].add(-moved).at[sink].add(moved)
    members = jnp.searchsorted(jnp.cumsum(sizes), jnp.arange(rows * top), side="right").astype(jnp.int32)
    listing = members.reshape(top, rows).T
    listing = listing[jax.random.permutation(jax.random.fold_in(own, 1), rows)]
    turn = jax.random.randint(jax.random.fold_in(own, 2), (rows, 1), 0, top)
    return jnp.take_along_axis(listing, (jnp.arange(top)[None, :] + turn) % top, axis=1)


def shares(number_of, total, limit, lean, full):
    loads = [(1 << 20) // math.isqrt(grade ** lean) + 1 for grade in range(1, number_of + 1)]
    largest = limit if full else min(limit, max(-(-total // number_of), total * loads[0] // sum(loads)))
    least = 1 if total - largest >= number_of - 1 else 0
    given, rest = [largest] + [least] * (number_of - 1), total - largest - least * (number_of - 1)
    while rest > 0:
        candidates = [i for i in range(1, number_of) if given[i] < largest] or [i for i in range(1, number_of) if given[i] < limit]
        mass, left = sum([loads[i] for i in candidates]), rest
        for i in candidates:
            extra = min(limit - given[i], max(1, left * loads[i] // mass), rest)
            given[i] = given[i] + extra
            rest = rest - extra
    return np.array(given)


def gaussian(rng, shape, scale, reach, shards=(), held_as=jnp.bfloat16):
    values = scale * jax.random.normal(rng, shape, jnp.float32)
    if shards:
        values = values * levels(rng, shape, shards, -0.22, 0.18)
    return jnp.clip(values, -reach, reach).astype(held_as)


def setup_inputs(seed: int = 0) -> dict:
    streams_of = jax.random.split(jax.random.key(seed), 14)
    track_embed = gaussian(streams_of[0], (TRACKS, D), 1.0, 6.0, ((0, 32),))
    view_ids_keys = jax.random.split(jax.random.fold_in(streams_of[1], 1), TRACKS // TRK_DEV)
    view_ids_turns = jax.random.permutation(jax.random.fold_in(streams_of[1], 3), TRACKS // TRK_DEV)
    view_ids = jax.vmap(lambda own, number: assign_block(jax.random.fold_in(streams_of[1], 2), own, number, TRK_DEV, FR_DEV * N_TM * CAMS, VMAX, CAP, 2))(view_ids_keys, view_ids_turns).reshape((TRACKS, VMAX))
    view_count = plant(jax.random.randint(streams_of[2], (TRACKS,), 1, VMAX + 1), jax.random.fold_in(streams_of[2], 1), 1, VMAX).astype(jnp.int32)
    key_feats = draw_key_feats(jax.random.fold_in(streams_of[13], 71), 0)
    value_feats = gaussian(streams_of[4], (FRAMES, CAMS, PIX, D), 1.0, 6.0, ((0, 8), (1, 4)))
    track_gain = jnp.clip(1.0 + 0.1 * jax.random.normal(streams_of[5], (D,), jnp.float32), 0.5, 1.5)
    w_temporal = gaussian(streams_of[6], (D, 3 * D), D ** -0.5, 0.1875)
    temporal_scale = draw_temporal_scale(jax.random.fold_in(streams_of[13], 71), 0)
    w_merge = gaussian(streams_of[8], (D, D), D ** -0.5, 0.1875)
    box_gain = jnp.clip(1.0 + 0.1 * jax.random.normal(streams_of[9], (D,), jnp.float32), 0.5, 1.5)
    w_hidden = gaussian(streams_of[10], (D, MLPW), D ** -0.5, 0.1875)
    b_hidden = gaussian(streams_of[11], (MLPW,), 1.0, 4.0, (), jnp.float32)
    w_box = gaussian(streams_of[12], (MLPW, BOX), MLPW ** -0.5, 0.25)
    return dict(track_embed=track_embed, view_ids=view_ids, view_count=view_count, key_feats=key_feats, value_feats=value_feats, track_gain=track_gain, w_temporal=w_temporal, temporal_scale=temporal_scale, w_merge=w_merge, box_gain=box_gain, w_hidden=w_hidden, b_hidden=b_hidden, w_box=w_box)


epsilon = 1e-05
masked_score = -1e+30

def layer_norm(values):
    centre = lax.optimization_barrier(jnp.mean(values, axis=-1, keepdims=True))
    shifted = values - centre
    spread = lax.optimization_barrier(jnp.mean(shifted * shifted, axis=-1, keepdims=True))
    return shifted * lax.rsqrt(spread + epsilon)

def time_code(frame_ids, model_width):
    half_width = model_width // 2
    freq_index = jnp.arange(half_width).astype(jnp.float32)
    freq_rates = jnp.exp(freq_index * (-2.0 * math.log(10000.0) / model_width))
    angles = frame_ids.astype(jnp.float32)[..., None] * freq_rates
    return jnp.concatenate([jnp.sin(angles), jnp.cos(angles)], axis=-1)

def view_attention(picked, key_rows, value_rows):
    row_count = picked.shape[0]
    head_feature_width = D // HEADS
    per_head_queries = picked.astype(jnp.float32).reshape(row_count, HEADS, head_feature_width)
    per_head_keys = key_rows.astype(jnp.float32).reshape(key_rows.shape[0], HEADS, head_feature_width)
    per_head_values = value_rows.astype(jnp.float32).reshape(value_rows.shape[0], HEADS, head_feature_width)
    attention_scores = jnp.einsum('ljk,fjk->jlf', per_head_queries, per_head_keys) * head_feature_width ** (-0.5)
    row_top = lax.optimization_barrier(jnp.max(attention_scores, axis=-1, keepdims=True))
    weights = jnp.exp(attention_scores - row_top)
    totals = lax.optimization_barrier(jnp.sum(weights, axis=-1))
    rounded_scores = lax.optimization_barrier(weights.astype(jnp.bfloat16)).astype(jnp.float32)
    softmax_numerator = jnp.einsum('tnz,ztr->ntr', rounded_scores, per_head_values)
    result_rows = softmax_numerator / jnp.transpose(totals)[:, :, None]
    return result_rows.reshape(row_count, D).astype(jnp.bfloat16)

def track_block(states, attended, counts, w_temporal, temporal_scale, w_merge, box_gain, w_hidden, b_hidden, w_box):
    track_rows = states.shape[0]
    list_length = attended.shape[1]
    model_width = states.shape[1]
    head_feature_width = model_width // HEADS
    residual_rows = states[:, None, :] + attended.astype(jnp.float32)
    normed = layer_norm(residual_rows).astype(jnp.bfloat16)
    projected = jnp.dot(normed.reshape(track_rows * list_length, model_width), w_temporal, preferred_element_type=jnp.float32).astype(jnp.bfloat16)
    projected = lax.optimization_barrier(projected)
    projected = projected.reshape(track_rows, list_length, 3, HEADS, head_feature_width).astype(jnp.float32)
    per_head_queries = projected[:, :, 0]
    per_head_keys = projected[:, :, 1]
    per_head_values = projected[:, :, 2]
    attention_scores = jnp.einsum('bqhd,bkhd->bhqk', per_head_queries, per_head_keys) * (temporal_scale[None, :, None, None] * head_feature_width ** (-0.5))
    positions = jnp.arange(list_length).astype(jnp.int32)
    key_valid = positions[None, :] < counts.astype(jnp.int32)[:, None]
    attention_scores = jnp.where(key_valid[:, None, None, :], attention_scores, masked_score)
    row_top = lax.optimization_barrier(jnp.max(attention_scores, axis=-1, keepdims=True))
    weights = jnp.exp(attention_scores - row_top)
    probs = (weights / lax.optimization_barrier(jnp.sum(weights, axis=-1, keepdims=True))).astype(jnp.bfloat16)
    probs = lax.optimization_barrier(probs).astype(jnp.float32)
    mixed_heads = jnp.einsum('bhqk,bkhd->bqhd', probs, per_head_values).astype(jnp.bfloat16)
    mixed_heads = mixed_heads.reshape(track_rows * list_length, model_width)
    updated = residual_rows + jnp.dot(mixed_heads, w_merge, preferred_element_type=jnp.float32).reshape(track_rows, list_length, model_width)
    row_valid = key_valid.astype(jnp.float32)[:, :, None]
    refined = (updated * row_valid).astype(jnp.bfloat16)
    box_input = (layer_norm(updated) * box_gain).astype(jnp.bfloat16)
    box_hidden = jax.nn.gelu(jnp.dot(box_input.reshape(track_rows * list_length, model_width), w_hidden, preferred_element_type=jnp.float32) + b_hidden).astype(jnp.bfloat16)
    box_values = jnp.dot(box_hidden, w_box, preferred_element_type=jnp.float32).reshape(track_rows, list_length, w_box.shape[1]) * row_valid
    return (refined, box_values)

def reference(track_embed, view_ids, view_count, key_feats, value_feats, track_gain, w_temporal, temporal_scale, w_merge, box_gain, w_hidden, b_hidden, w_box):
    tracks_total = track_embed.shape[0]
    states = layer_norm(track_embed.astype(jnp.float32)) * track_gain
    frame_ids = view_ids // CAMS
    queries = (states[:, None, :] + time_code(frame_ids, D)).astype(jnp.bfloat16)
    row_total = tracks_total * VMAX
    flat_queries = queries.reshape(row_total, D)
    flat_views = view_ids.reshape(row_total).astype(jnp.int32)
    per_view = CAP * N_TM * N_TRK
    view_total = FRAMES * CAMS

    def one_view(scan_carry, view_id):
        row_ids = jnp.nonzero(flat_views == view_id, size=per_view, fill_value=row_total)[0].astype(jnp.int32)
        frame_id = view_id // CAMS
        camera_id = view_id % CAMS
        neighbour = (camera_id + 1) % CAMS
        key_rows = jnp.concatenate([key_feats[frame_id, camera_id], key_feats[frame_id, neighbour]], axis=0)
        value_rows = jnp.concatenate([value_feats[frame_id, camera_id], value_feats[frame_id, neighbour]], axis=0)
        picked = jnp.take(flat_queries, row_ids, axis=0, mode='fill', fill_value=0)
        return (scan_carry, (row_ids, view_attention(picked, key_rows, value_rows)))
    scan_carry, outcome = lax.scan(one_view, jnp.int32(0), jnp.arange(view_total, dtype=jnp.int32))
    row_lists, results = outcome
    attended = jnp.zeros((row_total, D), jnp.bfloat16).at[row_lists.reshape(-1)].set(results.reshape(-1, D), mode='drop')
    blocks = tracks_total // TRK_DEV
    block_parts = (states.reshape(blocks, TRK_DEV, D), attended.reshape(blocks, TRK_DEV, VMAX, D), view_count.reshape(blocks, TRK_DEV))

    def one_block(parts_here):
        return track_block(parts_here[0], parts_here[1], parts_here[2], w_temporal, temporal_scale, w_merge, box_gain, w_hidden, b_hidden, w_box)
    refined, box_values = lax.map(one_block, block_parts)
    return (refined.reshape(tracks_total, VMAX, D), box_values.reshape(tracks_total, VMAX, BOX))
```

```python
import math

import jax
import jax.numpy as jnp
from jax import lax
from jax.experimental import pallas as pl
from jax.experimental.pallas import tpu as pltpu
from jax.sharding import PartitionSpec as P

HEADS = 8
CAMS = 8


epsilon = 1e-05
masked_score = -1e30


def from_behind(block, axis, distance):
    devices = range(lax.axis_size(axis))
    route = [((i - distance) % len(devices), i) for i in devices]
    return lax.ppermute(block, axis, route)


def layer_norm(values):
    centre = jnp.mean(values, axis=-1, keepdims=True)
    shifted = values - centre
    spread = jnp.mean(shifted * shifted, axis=-1, keepdims=True)
    return shifted * lax.rsqrt(spread + epsilon)


def time_code(frame_ids, model_width):
    half_width = model_width // 2
    freq_index = jnp.arange(half_width).astype(jnp.float32)
    freq_rates = jnp.exp(freq_index * (-2.0 * math.log(10000.0) / model_width))
    angles = frame_ids.astype(jnp.float32)[..., None] * freq_rates
    return jnp.concatenate([jnp.sin(angles), jnp.cos(angles)], axis=-1)


def exchange(block, axis, stride):
    size = lax.axis_size(axis)
    return lax.ppermute(block, axis, [(i, i ^ stride) for i in range(size)])


def gather_tracks(rows, split):
    tm_count = lax.axis_size("tm")
    trk_count = lax.axis_size("trk")
    masks = []
    for axis, size, unit, first in (("tm", tm_count, trk_count, 2), ("trk", trk_count, 1, 4)):
        stride = first
        while stride < size:
            rows = jnp.concatenate([rows, exchange(rows, axis, stride)], axis=0)
            masks.append(stride * unit)
            stride *= 2
    part = rows.shape[0]
    left, right = rows[:, :split], rows[:, split:]
    left_x, right_y = exchange(left, "tm", 1), exchange(right, "trk", 2)
    left = jnp.concatenate([left, left_x], axis=0)
    right = jnp.concatenate([right, right_y], axis=0)
    left_y, right_x = exchange(left, "trk", 2), exchange(right, "tm", 1)
    left = jnp.concatenate([left, left_y], axis=0)
    right = jnp.concatenate([right[:part], right_x[:part], right[part:], right_x[part:]], axis=0)
    masks += [trk_count, 2, 1]
    return left, exchange(left, "trk", 1), right, exchange(right, "trk", 1), masks


def iota(shape, axis):
    return lax.broadcasted_iota(jnp.int32, shape, axis)


def match_row(ids, view):
    hit = jnp.where(ids.astype(jnp.float32) == view, 1.0, 0.0).astype(jnp.bfloat16)
    ones = jnp.ones((8, ids.shape[1]), jnp.bfloat16)
    return lax.dot_general(ones, hit, (((1,), (1,)), ((), ())), preferred_element_type=jnp.float32)


def ranks_of(ids_refs, view, store, width):
    before = iota((width, width), 0) < iota((width, width), 1)
    before = jnp.where(before, 1.0, 0.0).astype(jnp.bfloat16)
    base = jnp.zeros((8, 1), jnp.float32)
    at = 0
    for ids_ref, columns in ids_refs:
        for low in range(0, ids_ref.shape[0], width):
            mask = match_row(ids_ref[low : low + width, columns], view)
            rank = base + jnp.dot(
                mask.astype(jnp.bfloat16), before, preferred_element_type=jnp.float32
            )
            store(at, mask, rank)
            base = base + jnp.sum(mask, axis=1, keepdims=True)
            at += width
    return base


def attend_kernel(
    info_ref,
    left0_ref,
    left1_ref,
    right0_ref,
    right1_ref,
    key0_ref,
    key1_ref,
    value0_ref,
    value1_ref,
    gain_ref,
    code_ref,
    out_ref,
    query_ref,
    rank_ref,
    count_ref,
    *,
    row_block,
    code_width,
):
    head = pl.program_id(0)
    rows_total, head_width = out_ref.shape
    chunks = rows_total // row_block
    model_width = gain_ref.shape[1]
    half = left0_ref.shape[1] - code_width
    tracks = left0_ref.shape[0]

    @pl.when(head == 0)
    def _():
        view = info_ref[0].astype(jnp.float32)

        def store(at, mask, rank):
            rank_ref[:, at : at + mask.shape[1]] = jnp.where(mask > 0.5, rank, -1.0)

        columns = slice(half, half + code_width)
        total = ranks_of(
            ((left0_ref, columns), (left1_ref, columns)), view, store, min(512, tracks)
        )
        count_ref[0] = (jnp.max(total).astype(jnp.int32) + row_block - 1) // row_block

        def one_chunk(c, carry):
            wanted = (iota((row_block, 1), 0) + c * row_block).astype(jnp.float32)
            low = jnp.zeros((row_block, half), jnp.float32)
            high = jnp.zeros((row_block, model_width - half), jnp.float32)
            for piece, (left_ref, right_ref) in enumerate(
                ((left0_ref, right0_ref), (left1_ref, right1_ref))
            ):
                ranks = rank_ref[0:1, piece * tracks : (piece + 1) * tracks]
                pick = jnp.where(ranks == wanted, 1.0, 0.0).astype(jnp.bfloat16)
                low += jnp.dot(pick, left_ref[:, :half], preferred_element_type=jnp.float32)
                high += jnp.dot(pick, right_ref[...], preferred_element_type=jnp.float32)
            rows = jnp.concatenate([low, high], axis=1)
            states = layer_norm(rows) * gain_ref[...]
            at = pl.multiple_of(c * row_block, row_block)
            query_ref[pl.ds(at, row_block), :] = (states + code_ref[...]).astype(jnp.bfloat16)
            return carry

        lax.fori_loop(0, count_ref[0], one_chunk, 0)

    scale = head_width ** (-0.5)
    keys = jnp.concatenate([key0_ref[...], key1_ref[...]], axis=0)
    values = jnp.concatenate([value0_ref[...], value1_ref[...]], axis=0)
    lane = pl.multiple_of(head * head_width, head_width)

    def one_chunk(c, carry):
        at = pl.multiple_of(c * row_block, row_block)
        query = query_ref[pl.ds(at, row_block), pl.ds(lane, head_width)]
        scores = lax.dot_general(
            query, keys, (((1,), (1,)), ((), ())), preferred_element_type=jnp.float32
        )
        top = jnp.max(scores, axis=1, keepdims=True)
        weights = jnp.exp((scores - top) * scale)
        totals = jnp.sum(weights, axis=1, keepdims=True)
        mixed = jnp.dot(weights.astype(jnp.bfloat16), values, preferred_element_type=jnp.float32)
        out_ref[pl.ds(at, row_block), :] = (mixed / totals).astype(jnp.bfloat16)
        return carry

    lax.fori_loop(0, count_ref[0], one_chunk, 0)

    def clear(c, carry):
        at = pl.multiple_of(c * row_block, row_block)
        out_ref[pl.ds(at, row_block), :] = jnp.zeros((row_block, head_width), jnp.bfloat16)
        return carry

    lax.fori_loop(count_ref[0], chunks, clear, 0)


def attend_view(info, gathered, keys, values, gain, code, rows_total, code_width):
    left0, left1, right0, right1 = gathered
    model_width = gain.shape[1]
    head_width = model_width // HEADS
    row_block = math.gcd(128, rows_total)
    whole = lambda a: pl.BlockSpec(a.shape, lambda h: (0,) * a.ndim)

    def part(array, frame, camera):
        return pl.BlockSpec(
            (None, None, array.shape[2], head_width), lambda h: (frame, camera, 0, h)
        )

    tokens = [k for k, _, _ in keys] + [v for v, _, _ in values]
    places = [part(*k) for k in keys] + [part(*v) for v in values]
    return pl.pallas_call(
        lambda *refs: attend_kernel(*refs, row_block=row_block, code_width=code_width),
        grid=(HEADS,),
        in_specs=[pl.BlockSpec(memory_space=pltpu.SMEM)]
        + [whole(a) for a in gathered]
        + places
        + [whole(gain), whole(code)],
        out_specs=pl.BlockSpec((rows_total, head_width), lambda h: (0, h)),
        out_shape=jax.ShapeDtypeStruct((rows_total, model_width), jnp.bfloat16),
        scratch_shapes=[
            pltpu.VMEM((rows_total, model_width), jnp.bfloat16),
            pltpu.VMEM((8, 2 * left0.shape[0]), jnp.float32),
            pltpu.SMEM((1,), jnp.int32),
        ],
        name="attend_view",
    )(info, *gathered, *tokens, gain, code)


def pack_kernel(info_ref, ids0_ref, ids1_ref, *refs, masks, block, capacity, views):
    results, out_ref, place_ref, rank_ref = refs[:views], refs[views], refs[views + 1], refs[-1]
    step = pl.program_id(0)
    tracks = ids0_ref.shape[0]
    width = min(512, tracks)
    rows_each = results[0].shape[0]

    @pl.when(step == 0)
    def _():
        same = iota((width, width), 0) // block == iota((width, width), 1) // block
        inside = same & (iota((width, width), 0) < iota((width, width), 1))
        same = jnp.where(same, 1.0, 0.0).astype(jnp.bfloat16)
        inside = jnp.where(inside, 1.0, 0.0).astype(jnp.bfloat16)
        taken = [0.0] * (2 * tracks // width)
        for v in range(views):

            def store(at, mask, rank):
                bits = mask.astype(jnp.bfloat16)
                spot = iota((8, width), 1) + at
                number = spot // block
                owner = jnp.full((8, width), info_ref[1], jnp.int32)
                for bit, mark in enumerate(masks):
                    owner = owner ^ (((number >> bit) & 1) * mark)
                place = taken[at // width] + jnp.dot(
                    bits, inside, preferred_element_type=jnp.float32
                )
                place = place + owner.astype(jnp.float32) * capacity
                chosen = mask > 0.5
                here = slice(at, at + width)
                place_ref[8 * v : 8 * v + 8, here] = jnp.where(chosen, place, -1.0)
                rank_ref[8 * v : 8 * v + 8, here] = jnp.where(
                    chosen, rank + (v * rows_each + 1), 0.0
                )
                taken[at // width] = taken[at // width] + jnp.dot(
                    bits, same, preferred_element_type=jnp.float32
                )

            ranks_of(
                ((ids0_ref, slice(None)), (ids1_ref, slice(None))),
                (info_ref[0] + v).astype(jnp.float32),
                store,
                width,
            )

    rows = out_ref.shape[0]
    slot = (iota((rows, 1), 0) + step * rows).astype(jnp.float32)
    source = jnp.zeros((rows, 1), jnp.float32)
    for v in range(views):
        hit = place_ref[8 * v : 8 * v + 1, :] == slot
        source += jnp.sum(
            jnp.where(hit, rank_ref[8 * v : 8 * v + 1, :], 0.0), axis=1, keepdims=True
        )
    packed = jnp.zeros(out_ref.shape, jnp.float32)
    for v in range(views):
        column = (iota((1, rows_each), 1) + (v * rows_each + 1)).astype(jnp.float32)
        pick = jnp.where(source == column, 1.0, 0.0).astype(jnp.bfloat16)
        packed += jnp.dot(pick, results[v][...], preferred_element_type=jnp.float32)
    out_ref[...] = packed.astype(jnp.bfloat16)


def pack_results(info, left0, left1, results, masks, block, capacity, code_width, slots):
    model_width = results[0].shape[1]
    views = len(results)
    tracks = left0.shape[0]
    last = left0.shape[1] // code_width - 1
    rows = math.gcd(256, slots)
    whole = lambda a: pl.BlockSpec(a.shape, lambda i: (0, 0))
    ids = pl.BlockSpec((tracks, code_width), lambda i: (0, last))
    return pl.pallas_call(
        lambda *refs: pack_kernel(
            *refs, masks=masks, block=block, capacity=capacity, views=views
        ),
        grid=(slots // rows,),
        in_specs=[pl.BlockSpec(memory_space=pltpu.SMEM), ids, ids] + [whole(r) for r in results],
        out_specs=pl.BlockSpec((rows, model_width), lambda i: (i, 0)),
        out_shape=jax.ShapeDtypeStruct((slots, model_width), jnp.bfloat16),
        scratch_shapes=[
            pltpu.VMEM((8 * views, 2 * tracks), jnp.float32),
            pltpu.VMEM((8 * views, 2 * tracks), jnp.float32),
        ],
        name="pack_results",
    )(info, left0, left1, *results)


def track_block(
    states,
    attended,
    counts,
    w_temporal,
    temporal_scale,
    w_merge,
    box_gain,
    w_hidden,
    b_hidden,
    w_box,
):
    track_rows = states.shape[0]
    list_length = attended.shape[1]
    model_width = states.shape[1]
    head_feature_width = model_width // HEADS
    residual_rows = states[:, None, :] + attended.astype(jnp.float32)
    normed = layer_norm(residual_rows).astype(jnp.bfloat16)
    projected = jnp.dot(
        normed.reshape(track_rows * list_length, model_width),
        w_temporal,
        preferred_element_type=jnp.float32,
    ).astype(jnp.bfloat16)
    projected = projected.reshape(track_rows, list_length, 3, HEADS, head_feature_width)
    per_head_queries = projected[:, :, 0]
    per_head_keys = projected[:, :, 1]
    per_head_values = projected[:, :, 2]
    attention_scores = jnp.einsum(
        "bqhd,bkhd->bhqk", per_head_queries, per_head_keys, preferred_element_type=jnp.float32
    )
    attention_scores = attention_scores * (
        temporal_scale[None, :, None, None] * head_feature_width ** (-0.5)
    )
    positions = jnp.arange(list_length)
    key_valid = positions[None, :] < counts[:, None]
    attention_scores = jnp.where(key_valid[:, None, None, :], attention_scores, masked_score)
    row_top = jnp.max(attention_scores, axis=-1, keepdims=True)
    weights = jnp.exp(attention_scores - row_top)
    probs = (weights / jnp.sum(weights, axis=-1, keepdims=True)).astype(jnp.bfloat16)
    mixed_heads = jnp.einsum(
        "bhqk,bkhd->bqhd", probs, per_head_values, preferred_element_type=jnp.float32
    ).astype(jnp.bfloat16)
    mixed_heads = mixed_heads.reshape(track_rows * list_length, model_width)
    updated = residual_rows + jnp.dot(
        mixed_heads, w_merge, preferred_element_type=jnp.float32
    ).reshape(track_rows, list_length, model_width)
    row_valid = key_valid.astype(jnp.float32)[:, :, None]
    refined = (updated * row_valid).astype(jnp.bfloat16)
    box_input = (layer_norm(updated) * box_gain).astype(jnp.bfloat16)
    box_hidden = jax.nn.gelu(
        jnp.dot(
            box_input.reshape(track_rows * list_length, model_width),
            w_hidden,
            preferred_element_type=jnp.float32,
        )
        + b_hidden
    ).astype(jnp.bfloat16)
    box_values = (
        jnp.dot(box_hidden, w_box, preferred_element_type=jnp.float32).reshape(
            track_rows, list_length, w_box.shape[1]
        )
        * row_valid
    )
    return (refined, box_values)


def local(
    track_embed,
    view_ids,
    view_count,
    key_feats,
    value_feats,
    track_gain,
    w_temporal,
    temporal_scale,
    w_merge,
    box_gain,
    w_hidden,
    b_hidden,
    w_box,
):
    tm_count = lax.axis_size("tm")
    trk_count = lax.axis_size("trk")
    device_count = tm_count * trk_count
    device = lax.axis_index("tm") * trk_count + lax.axis_index("trk")
    local_frames = key_feats.shape[0]
    local_cameras = key_feats.shape[1]
    model_width = track_embed.shape[1]
    track_local = track_embed.shape[0]
    list_length = view_ids.shape[1]
    row_local = track_local * list_length
    view_total = local_frames * tm_count * CAMS
    capacity = max(2, (2 * row_local + view_total - 1) // view_total)
    local_views = local_frames * local_cameras
    pair_rows = local_views * capacity
    code_width = 128

    valid = jnp.arange(list_length)[None, :] < view_count[:, None]
    frames = view_ids // CAMS
    cameras = view_ids % CAMS
    owner = frames // local_frames * trk_count + cameras // local_cameras
    ordered_view = owner * local_views + frames % local_frames * local_cameras
    ordered_view = ordered_view + cameras % local_cameras
    listed = jnp.where(valid, ordered_view, -1)

    tagged = jnp.pad(
        listed.astype(jnp.bfloat16), ((0, 0), (0, code_width - list_length)), constant_values=-1
    )
    half = model_width // 2
    tagged = jnp.concatenate([track_embed[:, :half], tagged, track_embed[:, half:]], axis=1)
    left0, left1, right0, right1, masks = gather_tracks(tagged, half + code_width)
    next_key, next_value = from_behind((key_feats[:, :1], value_feats[:, :1]), "trk", -1)

    gain = track_gain.reshape(1, model_width)
    gathered = (left0, left1, right0, right1)
    results = []
    first_view = device * local_views
    for frame in range(local_frames):
        frame_id = lax.axis_index("tm") * local_frames + frame
        code = time_code(frame_id.reshape(1), model_width)
        for camera in range(local_cameras):
            following = camera + 1
            if following < local_cameras:
                keys = [(key_feats, frame, camera), (key_feats, frame, following)]
                values = [(value_feats, frame, camera), (value_feats, frame, following)]
            else:
                keys = [(key_feats, frame, camera), (next_key, frame, 0)]
                values = [(value_feats, frame, camera), (next_value, frame, 0)]
            info = jnp.stack([first_view + len(results), device]).astype(jnp.int32)
            results.append(
                attend_view(
                    info, gathered, keys, values, gain, code, capacity * device_count, code_width
                )
            )
    info = jnp.stack([first_view, device]).astype(jnp.int32)
    outbound = pack_results(
        info,
        left0,
        left1,
        results,
        masks,
        track_local,
        pair_rows,
        code_width,
        device_count * pair_rows,
    )
    returned = lax.all_to_all(
        outbound.reshape(device_count, pair_rows, model_width),
        ("tm", "trk"),
        split_axis=0,
        concat_axis=0,
        tiled=True,
    )

    flat = listed.reshape(row_local)
    order = flat * track_local + jnp.arange(row_local, dtype=jnp.int32) // list_length
    source = flat // local_views
    ahead = (
        (source[None, :] == source[:, None])
        & (order[None, :] < order[:, None])
        & (flat >= 0)[None, :]
    )
    place = source * pair_rows + jnp.sum(ahead.astype(jnp.int32), axis=1)
    place = jnp.where(flat >= 0, place, -1)
    pick = (place[:, None] == jnp.arange(device_count * pair_rows)[None, :]).astype(jnp.bfloat16)
    attended = jnp.dot(
        pick,
        returned.reshape(device_count * pair_rows, model_width),
        preferred_element_type=jnp.float32,
    ).reshape(track_local, list_length, model_width)
    states = layer_norm(track_embed.astype(jnp.float32)) * track_gain
    return track_block(
        states,
        attended,
        view_count,
        w_temporal,
        temporal_scale,
        w_merge,
        box_gain,
        w_hidden,
        b_hidden,
        w_box,
    )


def solution(mesh):
    placed = (
        P(("tm", "trk"), None),
        P(("tm", "trk"), None),
        P(("tm", "trk")),
        P("tm", "trk", None, None),
        P("tm", "trk", None, None),
        P(),
        P(),
        P(),
        P(),
        P(),
        P(),
        P(),
        P(),
    )
    return jax.shard_map(
        local,
        mesh=mesh,
        in_specs=placed,
        out_specs=(P(("tm", "trk"), None, None), P(("tm", "trk"), None, None)),
        check_vma=False,
    )
```

```python
import math

import jax
import jax.numpy as jnp
from jax import lax
from jax.experimental import pallas as pl
from jax.experimental.pallas import tpu as pltpu
from jax.sharding import PartitionSpec as P

HEADS = 8
CAMS = 8


epsilon = 1e-05
masked_score = -1e30


def from_behind(block, axis, distance):
    devices = range(lax.axis_size(axis))
    route = [((i - distance) % len(devices), i) for i in devices]
    return lax.ppermute(block, axis, route)


def layer_norm(values):
    centre = jnp.mean(values, axis=-1, keepdims=True)
    shifted = values - centre
    spread = jnp.mean(shifted * shifted, axis=-1, keepdims=True)
    return shifted * lax.rsqrt(spread + epsilon)


def time_code(frame_ids, model_width):
    half_width = model_width // 2
    freq_index = jnp.arange(half_width).astype(jnp.float32)
    freq_rates = jnp.exp(freq_index * (-2.0 * math.log(10000.0) / model_width))
    angles = frame_ids.astype(jnp.float32)[..., None] * freq_rates
    return jnp.concatenate([jnp.sin(angles), jnp.cos(angles)], axis=-1)


ROW_BLOCK = 256
HEADS_AT_ONCE = 4


def exchange(block, axis, stride):
    size = lax.axis_size(axis)
    return lax.ppermute(block, axis, [(i, i ^ stride) for i in range(size)])


def gather_tracks(rows, split, sides):
    tm_count = lax.axis_size("tm")
    trk_count = lax.axis_size("trk")
    masks = []
    for axis, size, unit, first in (("tm", tm_count, trk_count, 2), ("trk", trk_count, 1, 4)):
        strides = []
        while first < size:
            strides.append(first)
            masks.append(first * unit)
            first *= 2
        for low in range(0, len(strides), 2):
            group = strides[low : low + 2]
            jumps = group + [sum(group)] * (len(group) - 1)
            rows = jnp.concatenate([rows] + [exchange(rows, axis, jump) for jump in jumps], axis=0)
    rows, sides = lax.optimization_barrier((rows, sides))
    part = rows.shape[0]
    left, right = rows[:, :split], rows[:, split:]
    left_x, right_y = exchange(left, "tm", 1), exchange(right, "trk", 2)
    left = jnp.concatenate([left, left_x], axis=0)
    right = jnp.concatenate([right, right_y], axis=0)
    left_y, right_x = exchange(left, "trk", 2), exchange(right, "tm", 1)
    left = jnp.concatenate([left, left_y], axis=0)
    right = jnp.concatenate([right[:part], right_x[:part], right[part:], right_x[part:]], axis=0)
    masks += [trk_count, 2, 1]
    return left, exchange(left, "trk", 1), right, exchange(right, "trk", 1), masks, sides


def iota(shape, axis):
    return lax.broadcasted_iota(jnp.int32, shape, axis)


def match_row(ids, view):
    hit = jnp.where(ids.astype(jnp.float32) == view, 1.0, 0.0).astype(jnp.bfloat16)
    ones = jnp.ones((8, ids.shape[1]), jnp.bfloat16)
    return lax.dot_general(ones, hit, (((1,), (1,)), ((), ())), preferred_element_type=jnp.float32)


def ranks_of(ids_refs, view, store, width):
    before = iota((width, width), 0) < iota((width, width), 1)
    before = jnp.where(before, 1.0, 0.0).astype(jnp.bfloat16)
    base = jnp.zeros((8, 1), jnp.float32)
    at = 0
    for ids_ref, columns in ids_refs:
        for low in range(0, ids_ref.shape[0], width):
            mask = match_row(ids_ref[low : low + width, columns], view)
            rank = base + jnp.dot(
                mask.astype(jnp.bfloat16), before, preferred_element_type=jnp.float32
            )
            store(at, mask, rank)
            base = base + jnp.sum(mask, axis=1, keepdims=True)
            at += width
    return base


def attend_kernel(
    info_ref,
    left0_ref,
    left1_ref,
    right0_ref,
    right1_ref,
    key0_ref,
    key1_ref,
    value0_ref,
    value1_ref,
    gain_ref,
    code_ref,
    out_ref,
    query_ref,
    rank_ref,
    place_ref,
    pack_ref,
    mixed_ref,
    count_ref,
    *,
    row_block,
    code_width,
    masks,
    block,
    capacity,
):
    head = pl.program_id(0)
    rows_total, step_width = out_ref.shape
    head_width = gain_ref.shape[1] // HEADS
    chunks = rows_total // row_block
    model_width = gain_ref.shape[1]
    half = left0_ref.shape[1] - code_width
    tracks = left0_ref.shape[0]

    @pl.when(head == 0)
    def _():
        view = info_ref[0].astype(jnp.float32)

        width = min(512, tracks)
        inside = (iota((width, width), 0) // block == iota((width, width), 1) // block) & (
            iota((width, width), 0) < iota((width, width), 1)
        )
        inside = jnp.where(inside, 1.0, 0.0).astype(jnp.bfloat16)

        def store(at, mask, rank):
            chosen = mask > 0.5
            here = slice(at, at + width)
            rank_ref[:, here] = jnp.where(chosen, rank, -1.0)
            number = (iota((8, width), 1) + at) // block
            owner = jnp.full((8, width), info_ref[1], jnp.int32)
            for bit, mark in enumerate(masks):
                owner = owner ^ (((number >> bit) & 1) * mark)
            place = jnp.dot(
                mask.astype(jnp.bfloat16), inside, preferred_element_type=jnp.float32
            )
            place = place + owner.astype(jnp.float32) * capacity
            place_ref[:, here] = jnp.where(chosen, place, -1.0)

        columns = slice(half, half + code_width)
        total = ranks_of(((left0_ref, columns), (left1_ref, columns)), view, store, width)
        count_ref[0] = (jnp.max(total).astype(jnp.int32) + row_block - 1) // row_block

        def one_chunk(c, carry):
            wanted = (iota((row_block, 1), 0) + c * row_block).astype(jnp.float32)
            low = jnp.zeros((row_block, half), jnp.float32)
            high = jnp.zeros((row_block, model_width - half), jnp.float32)
            for piece, (left_ref, right_ref) in enumerate(
                ((left0_ref, right0_ref), (left1_ref, right1_ref))
            ):
                ranks = rank_ref[0:1, piece * tracks : (piece + 1) * tracks]
                pick = jnp.where(ranks == wanted, 1.0, 0.0).astype(jnp.bfloat16)
                low += jnp.dot(pick, left_ref[:, :half], preferred_element_type=jnp.float32)
                high += jnp.dot(pick, right_ref[...], preferred_element_type=jnp.float32)
            rows = jnp.concatenate([low, high], axis=1)
            states = layer_norm(rows) * gain_ref[...]
            at = pl.multiple_of(c * row_block, row_block)
            query_ref[pl.ds(at, row_block), :] = (states + code_ref[...]).astype(jnp.bfloat16)
            return carry

        lax.fori_loop(0, count_ref[0], one_chunk, 0)
        mixed_ref[...] = jnp.zeros(mixed_ref.shape, jnp.bfloat16)
        column = (iota((1, rows_total), 1) + 1).astype(jnp.float32)

        def one_stretch(c, carry):
            at = pl.multiple_of(c * row_block, row_block)
            slot = (iota((row_block, 1), 0) + at).astype(jnp.float32)
            hit = place_ref[0:1, :] == slot
            source = jnp.sum(jnp.where(hit, rank_ref[0:1, :] + 1.0, 0.0), axis=1, keepdims=True)
            pick = jnp.where(source == column, 1.0, 0.0)
            pack_ref[pl.ds(at, row_block), :] = pick.astype(jnp.bfloat16)
            return carry

        lax.fori_loop(0, chunks, one_stretch, 0)

    scale = head_width ** (-0.5)
    lane = pl.multiple_of(head * step_width, step_width)
    across = (((1,), (1,)), ((), ()))

    def one_chunk(c, carry):
        at = pl.multiple_of(c * row_block, row_block)
        query = query_ref[pl.ds(at, row_block), pl.ds(lane, step_width)]
        for low in range(0, step_width, head_width):
            own = slice(low, low + head_width)
            scores0 = lax.dot_general(
                query[:, own], key0_ref[:, own], across, preferred_element_type=jnp.float32
            )
            scores1 = lax.dot_general(
                query[:, own], key1_ref[:, own], across, preferred_element_type=jnp.float32
            )
            top = jnp.max(jnp.maximum(scores0, scores1), axis=1, keepdims=True)
            weights0 = jnp.exp((scores0 - top) * scale)
            weights1 = jnp.exp((scores1 - top) * scale)
            totals = jnp.sum(weights0 + weights1, axis=1, keepdims=True)
            mixed = jnp.dot(
                weights0.astype(jnp.bfloat16), value0_ref[:, own], preferred_element_type=jnp.float32
            ) + jnp.dot(
                weights1.astype(jnp.bfloat16), value1_ref[:, own], preferred_element_type=jnp.float32
            )
            mixed_ref[pl.ds(at, row_block), own] = (mixed / totals).astype(jnp.bfloat16)
        return carry

    lax.fori_loop(0, count_ref[0], one_chunk, 0)

    def pack(used):
        out_ref[...] = jnp.dot(
            pack_ref[:, :used], mixed_ref[:used, :], preferred_element_type=jnp.float32
        ).astype(jnp.bfloat16)

    @pl.when(count_ref[0] <= 1)
    def _():
        pack(row_block)

    @pl.when(count_ref[0] > 1)
    def _():
        pack(rows_total)


def attend_view(info, gathered, keys, values, gain, code, capacity, code_width, masks, block):
    left0, _, _, _ = gathered
    model_width = gain.shape[1]
    step_width = model_width // HEADS * HEADS_AT_ONCE
    rows_total = capacity * 2 * left0.shape[0] // block
    row_block = math.gcd(ROW_BLOCK, rows_total)
    whole = lambda a: pl.BlockSpec(a.shape, lambda h: (0,) * a.ndim)

    def part(array, frame, camera):
        return pl.BlockSpec(
            (None, None, array.shape[2], step_width), lambda h: (frame, camera, 0, h)
        )

    tokens = [k for k, _, _ in keys] + [v for v, _, _ in values]
    places = [part(*k) for k in keys] + [part(*v) for v in values]
    return pl.pallas_call(
        lambda *refs: attend_kernel(
            *refs,
            row_block=row_block,
            code_width=code_width,
            masks=masks,
            block=block,
            capacity=capacity,
        ),
        grid=(HEADS // HEADS_AT_ONCE,),
        in_specs=[pl.BlockSpec(memory_space=pltpu.SMEM)]
        + [whole(a) for a in gathered]
        + places
        + [whole(gain), whole(code)],
        out_specs=pl.BlockSpec((rows_total, step_width), lambda h: (0, h)),
        out_shape=jax.ShapeDtypeStruct((rows_total, model_width), jnp.bfloat16),
        scratch_shapes=[
            pltpu.VMEM((rows_total, model_width), jnp.bfloat16),
            pltpu.VMEM((8, 2 * left0.shape[0]), jnp.float32),
            pltpu.VMEM((8, 2 * left0.shape[0]), jnp.float32),
            pltpu.VMEM((rows_total, rows_total), jnp.bfloat16),
            pltpu.VMEM((rows_total, step_width), jnp.bfloat16),
            pltpu.SMEM((1,), jnp.int32),
        ],
        cost_estimate=pl.CostEstimate(
            flops=8 * rows_total * 1024 * model_width, bytes_accessed=1 << 23, transcendentals=0
        ),
        name="attend_view",
    )(info, *gathered, *tokens, gain, code)


def track_block(
    states,
    attended,
    counts,
    w_temporal,
    temporal_scale,
    w_merge,
    box_gain,
    w_hidden,
    b_hidden,
    w_box,
):
    track_rows = states.shape[0]
    list_length = attended.shape[1]
    model_width = states.shape[1]
    head_feature_width = model_width // HEADS
    residual_rows = states[:, None, :] + attended.astype(jnp.float32)
    normed = layer_norm(residual_rows).astype(jnp.bfloat16)
    projected = jnp.dot(
        normed.reshape(track_rows * list_length, model_width),
        w_temporal,
        preferred_element_type=jnp.float32,
    ).astype(jnp.bfloat16)
    projected = projected.reshape(track_rows, list_length, 3, HEADS, head_feature_width)
    per_head_queries = projected[:, :, 0]
    per_head_keys = projected[:, :, 1]
    per_head_values = projected[:, :, 2]
    attention_scores = jnp.einsum(
        "bqhd,bkhd->bhqk", per_head_queries, per_head_keys, preferred_element_type=jnp.float32
    )
    attention_scores = attention_scores * (
        temporal_scale[None, :, None, None] * head_feature_width ** (-0.5)
    )
    positions = jnp.arange(list_length)
    key_valid = positions[None, :] < counts[:, None]
    attention_scores = jnp.where(key_valid[:, None, None, :], attention_scores, masked_score)
    row_top = jnp.max(attention_scores, axis=-1, keepdims=True)
    weights = jnp.exp(attention_scores - row_top)
    probs = (weights / jnp.sum(weights, axis=-1, keepdims=True)).astype(jnp.bfloat16)
    mixed_heads = jnp.einsum(
        "bhqk,bkhd->bqhd", probs, per_head_values, preferred_element_type=jnp.float32
    ).astype(jnp.bfloat16)
    mixed_heads = mixed_heads.reshape(track_rows * list_length, model_width)
    updated = residual_rows + jnp.dot(
        mixed_heads, w_merge, preferred_element_type=jnp.float32
    ).reshape(track_rows, list_length, model_width)
    row_valid = key_valid.astype(jnp.float32)[:, :, None]
    refined = (updated * row_valid).astype(jnp.bfloat16)
    box_input = (layer_norm(updated) * box_gain).astype(jnp.bfloat16)
    box_hidden = jax.nn.gelu(
        jnp.dot(
            box_input.reshape(track_rows * list_length, model_width),
            w_hidden,
            preferred_element_type=jnp.float32,
        )
        + b_hidden
    ).astype(jnp.bfloat16)
    box_values = (
        jnp.dot(box_hidden, w_box, preferred_element_type=jnp.float32).reshape(
            track_rows, list_length, w_box.shape[1]
        )
        * row_valid
    )
    return (refined, box_values)


def local(
    track_embed,
    view_ids,
    view_count,
    key_feats,
    value_feats,
    track_gain,
    w_temporal,
    temporal_scale,
    w_merge,
    box_gain,
    w_hidden,
    b_hidden,
    w_box,
):
    tm_count = lax.axis_size("tm")
    trk_count = lax.axis_size("trk")
    device_count = tm_count * trk_count
    device = lax.axis_index("tm") * trk_count + lax.axis_index("trk")
    local_frames = key_feats.shape[0]
    local_cameras = key_feats.shape[1]
    model_width = track_embed.shape[1]
    track_local = track_embed.shape[0]
    list_length = view_ids.shape[1]
    row_local = track_local * list_length
    view_total = local_frames * tm_count * CAMS
    capacity = max(2, (2 * row_local + view_total - 1) // view_total)
    local_views = local_frames * local_cameras
    code_width = 128

    valid = jnp.arange(list_length)[None, :] < view_count[:, None]
    frames = view_ids // CAMS
    cameras = view_ids % CAMS
    owner = frames // local_frames * trk_count + cameras // local_cameras
    ordered_view = owner * local_views + frames % local_frames * local_cameras
    ordered_view = ordered_view + cameras % local_cameras
    listed = jnp.where(valid, ordered_view, -1)

    tagged = jnp.pad(
        listed.astype(jnp.bfloat16), ((0, 0), (0, code_width - list_length)), constant_values=-1
    )
    half = model_width // 2
    tagged = jnp.concatenate([track_embed[:, :half], tagged, track_embed[:, half:]], axis=1)
    left0, left1, right0, right1, masks, firsts = gather_tracks(
        tagged, half + code_width, (key_feats[:, :1], value_feats[:, :1])
    )
    next_key = from_behind(firsts[0], "trk", -1)
    next_value = from_behind(firsts[1], "trk", -1)

    gain = track_gain.reshape(1, model_width)
    gathered = (left0, left1, right0, right1)
    returned = []
    first_view = device * local_views
    for frame in range(local_frames):
        frame_id = lax.axis_index("tm") * local_frames + frame
        code = time_code(frame_id.reshape(1), model_width)
        for camera in range(local_cameras):
            following = camera + 1
            if following < local_cameras:
                keys = [(key_feats, frame, camera), (key_feats, frame, following)]
                values = [(value_feats, frame, camera), (value_feats, frame, following)]
            else:
                keys = [(key_feats, frame, camera), (next_key, frame, 0)]
                values = [(value_feats, frame, camera), (next_value, frame, 0)]
            info = jnp.stack([first_view + len(returned), device]).astype(jnp.int32)
            outbound = attend_view(
                info, gathered, keys, values, gain, code, capacity, code_width, masks, track_local
            )
            outbound, first_view = lax.optimization_barrier((outbound, first_view))
            returned.append(
                lax.all_to_all(
                    outbound.reshape(device_count, capacity, model_width),
                    ("tm", "trk"),
                    split_axis=0,
                    concat_axis=0,
                    tiled=True,
                )
            )

    flat = listed.reshape(row_local)
    index = jnp.arange(row_local, dtype=jnp.int32)
    ahead = (flat[None, :] == flat[:, None]) & (index[None, :] < index[:, None])
    place = flat // local_views * capacity + jnp.sum(ahead.astype(jnp.int32), axis=1)
    slots = device_count * capacity
    attended = jnp.zeros((row_local, model_width), jnp.float32)
    for view, arrived in enumerate(returned):
        wanted = jnp.where((flat >= 0) & (flat % local_views == view), place, -1)
        pick = (wanted[:, None] == jnp.arange(slots)[None, :]).astype(jnp.bfloat16)
        attended += jnp.dot(
            pick, arrived.reshape(slots, model_width), preferred_element_type=jnp.float32
        )
    attended = attended.reshape(track_local, list_length, model_width)
    states = layer_norm(track_embed.astype(jnp.float32)) * track_gain
    return track_block(
        states,
        attended,
        view_count,
        w_temporal,
        temporal_scale,
        w_merge,
        box_gain,
        w_hidden,
        b_hidden,
        w_box,
    )


def solution(mesh):
    placed = (
        P(("tm", "trk"), None),
        P(("tm", "trk"), None),
        P(("tm", "trk")),
        P("tm", "trk", None, None),
        P("tm", "trk", None, None),
        P(),
        P(),
        P(),
        P(),
        P(),
        P(),
        P(),
        P(),
    )
    return jax.shard_map(
        local,
        mesh=mesh,
        in_specs=placed,
        out_specs=(P(("tm", "trk"), None, None), P(("tm", "trk"), None, None)),
        check_vma=False,
    )
```

```python
import math

import jax
import jax.numpy as jnp
from jax import lax
from jax.experimental import pallas as pl
from jax.experimental.pallas import tpu as pltpu
from jax.sharding import PartitionSpec as P

HEADS = 8
CAMS = 8


epsilon = 1e-05
masked_score = -1e30


def from_behind(block, axis, distance):
    devices = range(lax.axis_size(axis))
    route = [((i - distance) % len(devices), i) for i in devices]
    return lax.ppermute(block, axis, route)


def layer_norm(values):
    centre = jnp.mean(values, axis=-1, keepdims=True)
    shifted = values - centre
    spread = jnp.mean(shifted * shifted, axis=-1, keepdims=True)
    return shifted * lax.rsqrt(spread + epsilon)


def time_code(frame_ids, model_width):
    half_width = model_width // 2
    freq_index = jnp.arange(half_width).astype(jnp.float32)
    freq_rates = jnp.exp(freq_index * (-2.0 * math.log(10000.0) / model_width))
    angles = frame_ids.astype(jnp.float32)[..., None] * freq_rates
    return jnp.concatenate([jnp.sin(angles), jnp.cos(angles)], axis=-1)


ROW_BLOCK = 256
HEADS_AT_ONCE = 4
TRACK_BLOCK = 32


def exchange(block, axis, stride):
    size = lax.axis_size(axis)
    return lax.ppermute(block, axis, [(i, i ^ stride) for i in range(size)])


def gather_tracks(rows, split, sides):
    tm_count = lax.axis_size("tm")
    trk_count = lax.axis_size("trk")
    masks = []
    for axis, size, unit, first in (("tm", tm_count, trk_count, 2), ("trk", trk_count, 1, 4)):
        strides = []
        while first < size:
            strides.append(first)
            masks.append(first * unit)
            first *= 2
        for low in range(0, len(strides), 2):
            group = strides[low : low + 2]
            jumps = group + [sum(group)] * (len(group) - 1)
            rows = jnp.concatenate([rows] + [exchange(rows, axis, jump) for jump in jumps], axis=0)
    rows, sides = lax.optimization_barrier((rows, sides))
    part = rows.shape[0]
    left, right = rows[:, :split], rows[:, split:]
    left_x, right_y = exchange(left, "tm", 1), exchange(right, "trk", 2)
    left = jnp.concatenate([left, left_x], axis=0)
    right = jnp.concatenate([right, right_y], axis=0)
    left_y, right_x = exchange(left, "trk", 2), exchange(right, "tm", 1)
    left = jnp.concatenate([left, left_y], axis=0)
    right = jnp.concatenate([right[:part], right_x[:part], right[part:], right_x[part:]], axis=0)
    masks += [trk_count, 2, 1]
    return left, exchange(left, "trk", 1), right, exchange(right, "trk", 1), masks, sides


def iota(shape, axis):
    return lax.broadcasted_iota(jnp.int32, shape, axis)


def match_row(ids, view):
    hit = jnp.where(ids.astype(jnp.float32) == view, 1.0, 0.0).astype(jnp.bfloat16)
    ones = jnp.ones((8, ids.shape[1]), jnp.bfloat16)
    return lax.dot_general(ones, hit, (((1,), (1,)), ((), ())), preferred_element_type=jnp.float32)


def ranks_of(ids_refs, view, store, width):
    before = iota((width, width), 0) < iota((width, width), 1)
    before = jnp.where(before, 1.0, 0.0).astype(jnp.bfloat16)
    base = jnp.zeros((8, 1), jnp.float32)
    at = 0
    for ids_ref, columns in ids_refs:
        for low in range(0, ids_ref.shape[0], width):
            mask = match_row(ids_ref[low : low + width, columns], view)
            rank = base + jnp.dot(
                mask.astype(jnp.bfloat16), before, preferred_element_type=jnp.float32
            )
            store(at, mask, rank)
            base = base + jnp.sum(mask, axis=1, keepdims=True)
            at += width
    return base


def attend_kernel(
    info_ref,
    left0_ref,
    left1_ref,
    right0_ref,
    right1_ref,
    key0_ref,
    key1_ref,
    value0_ref,
    value1_ref,
    gain_ref,
    code_ref,
    out_ref,
    query_ref,
    rank_ref,
    place_ref,
    pack_ref,
    mixed_ref,
    count_ref,
    *,
    row_block,
    code_width,
    masks,
    block,
    capacity,
):
    head = pl.program_id(0)
    rows_total, step_width = out_ref.shape
    head_width = gain_ref.shape[1] // HEADS
    chunks = rows_total // row_block
    model_width = gain_ref.shape[1]
    half = left0_ref.shape[1] - code_width
    tracks = left0_ref.shape[0]

    @pl.when(head == 0)
    def _():
        view = info_ref[0].astype(jnp.float32)

        width = min(512, tracks)
        inside = (iota((width, width), 0) // block == iota((width, width), 1) // block) & (
            iota((width, width), 0) < iota((width, width), 1)
        )
        inside = jnp.where(inside, 1.0, 0.0).astype(jnp.bfloat16)

        def store(at, mask, rank):
            chosen = mask > 0.5
            here = slice(at, at + width)
            rank_ref[:, here] = jnp.where(chosen, rank, -1.0)
            number = (iota((8, width), 1) + at) // block
            owner = jnp.full((8, width), info_ref[1], jnp.int32)
            for bit, mark in enumerate(masks):
                owner = owner ^ (((number >> bit) & 1) * mark)
            place = jnp.dot(
                mask.astype(jnp.bfloat16), inside, preferred_element_type=jnp.float32
            )
            place = place + owner.astype(jnp.float32) * capacity
            place_ref[:, here] = jnp.where(chosen, place, -1.0)

        columns = slice(half, half + code_width)
        total = ranks_of(((left0_ref, columns), (left1_ref, columns)), view, store, width)
        count_ref[0] = (jnp.max(total).astype(jnp.int32) + row_block - 1) // row_block

        def one_chunk(c, carry):
            wanted = (iota((row_block, 1), 0) + c * row_block).astype(jnp.float32)
            low = jnp.zeros((row_block, half), jnp.float32)
            high = jnp.zeros((row_block, model_width - half), jnp.float32)
            for piece, (left_ref, right_ref) in enumerate(
                ((left0_ref, right0_ref), (left1_ref, right1_ref))
            ):
                ranks = rank_ref[0:1, piece * tracks : (piece + 1) * tracks]
                pick = jnp.where(ranks == wanted, 1.0, 0.0).astype(jnp.bfloat16)
                low += jnp.dot(pick, left_ref[:, :half], preferred_element_type=jnp.float32)
                high += jnp.dot(pick, right_ref[...], preferred_element_type=jnp.float32)
            rows = jnp.concatenate([low, high], axis=1)
            states = layer_norm(rows) * gain_ref[...]
            at = pl.multiple_of(c * row_block, row_block)
            query_ref[pl.ds(at, row_block), :] = (states + code_ref[...]).astype(jnp.bfloat16)
            return carry

        lax.fori_loop(0, count_ref[0], one_chunk, 0)
        mixed_ref[...] = jnp.zeros(mixed_ref.shape, jnp.bfloat16)
        column = (iota((1, rows_total), 1) + 1).astype(jnp.float32)

        def one_stretch(c, carry):
            at = pl.multiple_of(c * row_block, row_block)
            slot = (iota((row_block, 1), 0) + at).astype(jnp.float32)
            hit = place_ref[0:1, :] == slot
            source = jnp.sum(jnp.where(hit, rank_ref[0:1, :] + 1.0, 0.0), axis=1, keepdims=True)
            pick = jnp.where(source == column, 1.0, 0.0)
            pack_ref[pl.ds(at, row_block), :] = pick.astype(jnp.bfloat16)
            return carry

        lax.fori_loop(0, chunks, one_stretch, 0)

    scale = head_width ** (-0.5)
    lane = pl.multiple_of(head * step_width, step_width)
    across = (((1,), (1,)), ((), ()))

    def one_chunk(c, carry):
        at = pl.multiple_of(c * row_block, row_block)
        query = query_ref[pl.ds(at, row_block), pl.ds(lane, step_width)]
        for low in range(0, step_width, head_width):
            own = slice(low, low + head_width)
            scores0 = lax.dot_general(
                query[:, own], key0_ref[:, own], across, preferred_element_type=jnp.float32
            )
            scores1 = lax.dot_general(
                query[:, own], key1_ref[:, own], across, preferred_element_type=jnp.float32
            )
            top = jnp.max(jnp.maximum(scores0, scores1), axis=1, keepdims=True)
            weights0 = jnp.exp((scores0 - top) * scale)
            weights1 = jnp.exp((scores1 - top) * scale)
            totals = jnp.sum(weights0 + weights1, axis=1, keepdims=True)
            mixed = jnp.dot(
                weights0.astype(jnp.bfloat16), value0_ref[:, own], preferred_element_type=jnp.float32
            ) + jnp.dot(
                weights1.astype(jnp.bfloat16), value1_ref[:, own], preferred_element_type=jnp.float32
            )
            mixed_ref[pl.ds(at, row_block), own] = (mixed / totals).astype(jnp.bfloat16)
        return carry

    lax.fori_loop(0, count_ref[0], one_chunk, 0)

    def pack(used):
        out_ref[...] = jnp.dot(
            pack_ref[:, :used], mixed_ref[:used, :], preferred_element_type=jnp.float32
        ).astype(jnp.bfloat16)

    @pl.when(count_ref[0] <= 1)
    def _():
        pack(row_block)

    @pl.when(count_ref[0] == 2)
    def _():
        pack(min(2 * row_block, rows_total))

    @pl.when(count_ref[0] > 2)
    def _():
        pack(rows_total)


def attend_view(info, gathered, keys, values, gain, code, capacity, code_width, masks, block):
    left0, _, _, _ = gathered
    model_width = gain.shape[1]
    step_width = model_width // HEADS * HEADS_AT_ONCE
    rows_total = capacity * 2 * left0.shape[0] // block
    row_block = math.gcd(ROW_BLOCK, rows_total)
    whole = lambda a: pl.BlockSpec(a.shape, lambda h: (0,) * a.ndim)

    def part(array, frame, camera):
        return pl.BlockSpec(
            (None, None, array.shape[2], step_width), lambda h: (frame, camera, 0, h)
        )

    tokens = [k for k, _, _ in keys] + [v for v, _, _ in values]
    places = [part(*k) for k in keys] + [part(*v) for v in values]
    return pl.pallas_call(
        lambda *refs: attend_kernel(
            *refs,
            row_block=row_block,
            code_width=code_width,
            masks=masks,
            block=block,
            capacity=capacity,
        ),
        grid=(HEADS // HEADS_AT_ONCE,),
        in_specs=[pl.BlockSpec(memory_space=pltpu.SMEM)]
        + [whole(a) for a in gathered]
        + places
        + [whole(gain), whole(code)],
        out_specs=pl.BlockSpec((rows_total, step_width), lambda h: (0, h)),
        out_shape=jax.ShapeDtypeStruct((rows_total, model_width), jnp.bfloat16),
        scratch_shapes=[
            pltpu.VMEM((rows_total, model_width), jnp.bfloat16),
            pltpu.VMEM((8, 2 * left0.shape[0]), jnp.float32),
            pltpu.VMEM((8, 2 * left0.shape[0]), jnp.float32),
            pltpu.VMEM((rows_total, rows_total), jnp.bfloat16),
            pltpu.VMEM((rows_total, step_width), jnp.bfloat16),
            pltpu.SMEM((1,), jnp.int32),
        ],
        cost_estimate=pl.CostEstimate(
            flops=8 * rows_total * 1024 * model_width, bytes_accessed=1 << 23, transcendentals=0
        ),
        name="attend_view",
    )(info, *gathered, *tokens, gain, code)


def track_kernel(
    *refs,
    views,
    list_length,
):
    (
        scale_ref,
        states_ref,
        place_ref,
        counts_ref,
        key_counts_ref,
    ) = refs[:5]
    arrived = refs[5 : 5 + views]
    (
        w_temporal_ref,
        w_merge_ref,
        box_gain_ref,
        w_hidden_ref,
        b_hidden_ref,
        w_box_ref,
        refined_ref,
        boxes_ref,
        mixed_ref,
    ) = refs[5 + views :]
    rows, model_width = refined_ref.shape
    head_width = model_width // HEADS
    attended = jnp.zeros((rows, model_width), jnp.float32)
    for v in range(views):
        slots = arrived[v].shape[0]
        pick = jnp.where(place_ref[:, v : v + 1] == iota((rows, slots), 1), 1.0, 0.0)
        attended += jnp.dot(
            pick.astype(jnp.bfloat16), arrived[v][...], preferred_element_type=jnp.float32
        )
    attended = attended.reshape(rows // list_length, list_length, model_width)
    residual = (states_ref[...][:, None, :] + attended).reshape(rows, model_width)
    normed = layer_norm(residual).astype(jnp.bfloat16)
    projected = jnp.dot(
        normed, w_temporal_ref[...], preferred_element_type=jnp.float32
    ).astype(jnp.bfloat16)
    small = math.gcd(rows, 128)
    row, column = iota((small, small), 0), iota((small, small), 1)
    same = row // list_length == column // list_length
    pieces = [(slice(low, low + small), head) for low in range(0, rows, small) for head in range(HEADS)]

    def columns(array, here, block, head):
        at = block * model_width + head * head_width
        return array[here, at : at + head_width]

    scores = []
    for here, head in pieces:
        score = lax.dot_general(
            columns(projected, here, 0, head),
            columns(projected, here, 1, head),
            (((1,), (1,)), ((), ())),
            preferred_element_type=jnp.float32,
        )
        score = score * (scale_ref[head] * head_width ** (-0.5))
        included = same & (column % list_length < key_counts_ref[:, here])
        scores.append(jnp.where(included, score, masked_score))
    scores = jnp.concatenate(scores, axis=0)
    weights = jnp.exp(scores - jnp.max(scores, axis=1, keepdims=True))
    probs = (weights / jnp.sum(weights, axis=1, keepdims=True)).astype(jnp.bfloat16)
    for number, (here, head) in enumerate(pieces):
        mixed_ref[here, head * head_width : (head + 1) * head_width] = jnp.dot(
            probs[number * small : (number + 1) * small],
            columns(projected, here, 2, head),
            preferred_element_type=jnp.float32,
        ).astype(jnp.bfloat16)
    updated = residual + jnp.dot(
        mixed_ref[...], w_merge_ref[...], preferred_element_type=jnp.float32
    )
    shown = jnp.where(iota((rows, 1), 0) % list_length < counts_ref[...], 1.0, 0.0)
    refined_ref[...] = (updated * shown).astype(jnp.bfloat16)
    box_input = (layer_norm(updated) * box_gain_ref[...]).astype(jnp.bfloat16)
    hidden = jnp.dot(box_input, w_hidden_ref[...], preferred_element_type=jnp.float32)
    hidden = hidden + b_hidden_ref[...]
    cubic = hidden + 0.044715 * (hidden * hidden * hidden)
    hidden = 0.5 * hidden * (1.0 + jnp.tanh(math.sqrt(2.0 / math.pi) * cubic))
    boxes = jnp.dot(
        hidden.astype(jnp.bfloat16), w_box_ref[...], preferred_element_type=jnp.float32
    )
    boxes_ref[...] = (boxes * shown).reshape(boxes_ref.shape)


def track_rows(
    states, places, counts, arrived, w_temporal, temporal_scale, w_merge, box_gain, w_hidden, b_hidden, w_box
):
    row_total = places.shape[0]
    track_total, model_width = states.shape
    list_length = row_total // track_total
    tracks = math.gcd(TRACK_BLOCK, track_total)
    rows = tracks * list_length
    whole = lambda a: pl.BlockSpec(a.shape, lambda i: (0, 0))
    by_row = lambda width, height=rows: pl.BlockSpec((height, width), lambda i: (i, 0))
    row_counts = jnp.repeat(counts, list_length)
    operands = [
        temporal_scale,
        states,
        places,
        row_counts.reshape(row_total, 1),
        row_counts.reshape(1, row_total),
        *arrived,
        w_temporal,
        w_merge,
        box_gain.reshape(1, -1),
        w_hidden,
        b_hidden.reshape(1, -1),
        w_box,
    ]
    specs = [
        pl.BlockSpec(memory_space=pltpu.SMEM),
        by_row(model_width, tracks),
        by_row(places.shape[1]),
        by_row(1),
        pl.BlockSpec((1, rows), lambda i: (0, i)),
    ] + [whole(a) for a in operands[5:]]
    return pl.pallas_call(
        lambda *refs: track_kernel(*refs, views=len(arrived), list_length=list_length),
        grid=(row_total // rows,),
        in_specs=specs,
        out_specs=[
            by_row(model_width),
            pl.BlockSpec((tracks, list_length, w_box.shape[1]), lambda i: (i, 0, 0)),
        ],
        out_shape=[
            jax.ShapeDtypeStruct((row_total, model_width), jnp.bfloat16),
            jax.ShapeDtypeStruct((track_total, list_length, w_box.shape[1]), jnp.float32),
        ],
        scratch_shapes=[pltpu.VMEM((rows, model_width), jnp.bfloat16)],
        name="track_rows",
    )(*operands)


def local(
    track_embed,
    view_ids,
    view_count,
    key_feats,
    value_feats,
    track_gain,
    w_temporal,
    temporal_scale,
    w_merge,
    box_gain,
    w_hidden,
    b_hidden,
    w_box,
):
    tm_count = lax.axis_size("tm")
    trk_count = lax.axis_size("trk")
    device_count = tm_count * trk_count
    device = lax.axis_index("tm") * trk_count + lax.axis_index("trk")
    local_frames = key_feats.shape[0]
    local_cameras = key_feats.shape[1]
    model_width = track_embed.shape[1]
    track_local = track_embed.shape[0]
    list_length = view_ids.shape[1]
    row_local = track_local * list_length
    view_total = local_frames * tm_count * CAMS
    capacity = max(2, (2 * row_local + view_total - 1) // view_total)
    local_views = local_frames * local_cameras
    code_width = 128

    valid = jnp.arange(list_length)[None, :] < view_count[:, None]
    frames = view_ids // CAMS
    cameras = view_ids % CAMS
    owner = frames // local_frames * trk_count + cameras // local_cameras
    ordered_view = owner * local_views + frames % local_frames * local_cameras
    ordered_view = ordered_view + cameras % local_cameras
    listed = jnp.where(valid, ordered_view, -1)

    tagged = jnp.pad(
        listed.astype(jnp.bfloat16), ((0, 0), (0, code_width - list_length)), constant_values=-1
    )
    half = model_width // 2
    tagged = jnp.concatenate([track_embed[:, :half], tagged, track_embed[:, half:]], axis=1)
    left0, left1, right0, right1, masks, firsts = gather_tracks(
        tagged, half + code_width, (key_feats[:, :1], value_feats[:, :1])
    )
    next_key = from_behind(firsts[0], "trk", -1)
    next_value = from_behind(firsts[1], "trk", -1)

    gain = track_gain.reshape(1, model_width)
    gathered = (left0, left1, right0, right1)
    returned = []
    first_view = device * local_views
    for frame in range(local_frames):
        frame_id = lax.axis_index("tm") * local_frames + frame
        code = time_code(frame_id.reshape(1), model_width)
        for camera in range(local_cameras):
            following = camera + 1
            if following < local_cameras:
                keys = [(key_feats, frame, camera), (key_feats, frame, following)]
                values = [(value_feats, frame, camera), (value_feats, frame, following)]
            else:
                keys = [(key_feats, frame, camera), (next_key, frame, 0)]
                values = [(value_feats, frame, camera), (next_value, frame, 0)]
            info = jnp.stack([first_view + len(returned), device]).astype(jnp.int32)
            outbound = attend_view(
                info, gathered, keys, values, gain, code, capacity, code_width, masks, track_local
            )
            outbound, first_view = lax.optimization_barrier((outbound, first_view))
            returned.append(
                lax.all_to_all(
                    outbound.reshape(device_count, capacity, model_width),
                    ("tm", "trk"),
                    split_axis=0,
                    concat_axis=0,
                    tiled=True,
                )
            )

    flat = listed.reshape(row_local)
    index = jnp.arange(row_local, dtype=jnp.int32)
    ahead = (flat[None, :] == flat[:, None]) & (index[None, :] < index[:, None])
    place = flat // local_views * capacity + jnp.sum(ahead.astype(jnp.int32), axis=1)
    places = [
        jnp.where((flat >= 0) & (flat % local_views == view), place, -1)
        for view in range(len(returned))
    ]
    states = layer_norm(track_embed.astype(jnp.float32)) * track_gain
    refined, boxes = track_rows(
        states,
        jnp.stack(places, axis=1),
        view_count,
        [arrived.reshape(-1, model_width) for arrived in returned],
        w_temporal,
        temporal_scale,
        w_merge,
        box_gain,
        w_hidden,
        b_hidden,
        w_box,
    )
    return (
        refined.reshape(track_local, list_length, model_width),
        boxes,
    )


def solution(mesh):
    placed = (
        P(("tm", "trk"), None),
        P(("tm", "trk"), None),
        P(("tm", "trk")),
        P("tm", "trk", None, None),
        P("tm", "trk", None, None),
        P(),
        P(),
        P(),
        P(),
        P(),
        P(),
        P(),
        P(),
    )
    return jax.shard_map(
        local,
        mesh=mesh,
        in_specs=placed,
        out_specs=(P(("tm", "trk"), None, None), P(("tm", "trk"), None, None)),
        check_vma=False,
    )
```
